32 devices in a mesh: dp: 2 (over x), tp: 16 (over y, z, core).
Axes of the slice: x: 2, y: 2, z: 4, core: 2. Of those that a mesh axis runs over, the one named last changes fastest.
Arguments:
- x: bfloat16 [4096, 5120], P('dp'), parts along dimension 0
- w_gate: bfloat16 [5120, 16384], P(None, 'tp')
- w_up: bfloat16 [5120, 16384], P(None, 'tp')
- w_down: bfloat16 [16384, 5120], P('tp')
Outputs:
- output: bfloat16 [4096, 5120], P('dp'), parts along dimension 0
There are 2 independent parts. The reference program is written for one: setup_inputs(seed, part) draws one part's arguments, and reference() takes and returns one part's arrays. A program takes and returns all parts, laid end to end along the dimension named above; an argument that names none is the same for every part.
All inputs are finite; a program needn't handle non-finite values.
Results may differ from the reference program's by a relative error of at most 0.016.
Values are sent between devices in bfloat16 or wider.
A program may use at most 2 GiB of HBM per device.

```python
import jax
import jax.numpy as jnp

ROWS = 2048
D = 5120
FF = 16384


def setup_inputs(seed: int = 0, part: int = 0) -> dict:
    kx, kg, ku, kd = jax.random.split(jax.random.key(seed), 4)
    drawn = {
        "x": jax.random.normal(jax.random.fold_in(kx, part), (ROWS, D), jnp.float32),
        "w_gate": jax.random.normal(kg, (D, FF), jnp.float32) * D**-0.5,
        "w_up": jax.random.normal(ku, (D, FF), jnp.float32) * D**-0.5,
        "w_down": jax.random.normal(kd, (FF, D), jnp.float32) * FF**-0.5,
    }
    return {k: v.astype(jnp.bfloat16) for k, v in drawn.items()}


def reference(x, w_gate, w_up, w_down):
    gate = jnp.dot(x, w_gate, preferred_element_type=jnp.float32)
    up = jnp.dot(x, w_up, preferred_element_type=jnp.float32)
    hidden = (jax.nn.silu(gate) * up).astype(jnp.bfloat16)
    return jnp.dot(hidden, w_down, preferred_element_type=jnp.float32).astype(jnp.bfloat16)
```

```python
import functools

import jax
import jax.numpy as jnp
from jax import lax
from jax.experimental import pallas as pl
from jax.experimental.pallas import tpu as pltpu
from jax.sharding import PartitionSpec as P

MESH = pl.DeviceIdType.MESH
CHIPS = 8
SUBS = 4
F32 = jnp.float32
BF16 = jnp.bfloat16


def block_kernel(x, wg, wu, wd, out, wg_v, wu_v, wd_v, xb, acc, theirs, d2d, hid,
                 w_sem, x_sem, d2d_send, d2d_recv, rs_send, rs_recv,
                 ag_send, ag_recv, pair_send, pair_recv):
    rows, depth = x.shape
    ff = wg.shape[1]
    cols = wd.shape[1]
    block = rows // CHIPS
    half = block // 2
    quarter = half // 2
    sub = quarter // SUBS
    gu_n = ff // SUBS

    tp = lax.axis_index("tp")
    core = tp % 2
    chip = tp // 2
    place = chip + (chip // 4) * (11 - 2 * chip)

    def at_place(k):
        k = k % CHIPS
        return 2 * (k + (k // 4) * (11 - 2 * k)) + core

    ring = (at_place(place + 1), at_place(place + CHIPS - 1))
    sibling = tp + 1 - 2 * core

    def block_of(d, s):
        if d == 0:
            return (place + 2 * CHIPS - 1 - s) % CHIPS
        return (place + 1 + s) % CHIPS

    def first_row(d, s, c):
        return block_of(d, s) * block + d * half + c * quarter

    def piece(d, s, j):
        return pl.ds(pl.multiple_of(first_row(d, s, core) + sub * j, sub), sub)

    def remote(src, dst, send, recv, device):
        return pltpu.make_async_remote_copy(
            src_ref=src, dst_ref=dst, send_sem=send, recv_sem=recv,
            device_id={"tp": device}, device_id_type=MESH)

    def x_copy(s, k):
        d, other = k % 2, k // 2
        c = core if other == 0 else 1 - core
        start = pl.multiple_of(first_row(d, s, c), quarter)
        return pltpu.make_async_copy(
            x.at[pl.ds(start, quarter), :], xb.at[pl.ds(k * quarter, quarter), :], x_sem.at[k])

    def w_copy(k, j):
        n = pl.ds(pl.multiple_of(j * gu_n, gu_n), gu_n)
        src, dst = ((wg, wg_v), (wu, wu_v))[k]
        return pltpu.make_async_copy(src.at[:, n], dst.at[:, n], w_sem.at[k, j])

    def wd_copy():
        return pltpu.make_async_copy(wd, wd_v, w_sem.at[2, 0])

    def d2d_copy(s):
        return remote(theirs, d2d.at[s % 2], d2d_send.at[0], d2d_recv.at[s % 2], sibling)

    def rs_copy(d, s, j):
        r = piece(d, s, j)
        return remote(out.at[r, :], out.at[r, :], rs_send.at[d, s, j], rs_recv.at[d, s, j], ring[d])

    def ag_copy(d, t, j):
        r = piece(d, t + CHIPS - 1, j)
        return remote(out.at[r, :], out.at[r, :], ag_send.at[d, t, j], ag_recv.at[d, t, j], ring[d])

    def pair_copy(d, t, j, c):
        r = pl.ds(pl.multiple_of(first_row(d, t + CHIPS - 1, c) + sub * j, sub), sub)
        return remote(out.at[r, :], out.at[r, :], pair_send.at[d, t, j], pair_recv.at[d, t, j], sibling)

    for k in range(4):
        x_copy(0, k).start()
    for j in range(SUBS):
        w_copy(0, j).start()
        w_copy(1, j).start()
    wd_copy().start()

    barrier = pltpu.get_barrier_semaphore()
    for device in (*ring, sibling):
        pl.semaphore_signal(barrier, inc=1, device_id={"tp": device}, device_id_type=MESH)
    pl.semaphore_wait(barrier, 3)

    def own_and_sibling(d, s, j):
        r = pl.ds(pl.multiple_of(d * quarter + sub * j, sub), sub)
        return acc[r, :] + d2d[s % 2, r, :].astype(F32)

    def combine(s, j):
        for d in range(2):
            rs_copy(d, s - 1, j).wait_send()
            pltpu.make_async_remote_copy(
                src_ref=out.at[piece(d, s, j), :], dst_ref=out.at[piece(d, s, j), :],
                send_sem=rs_send.at[d, s - 1, j], recv_sem=rs_recv.at[d, s - 1, j],
                device_id={"tp": ring[d]}, device_id_type=MESH).wait_recv()
            r = piece(d, s, j)
            out[r, :] = (own_and_sibling(d, s, j) + out[r, :].astype(F32)).astype(BF16)

    def comm(s, j):
        @pl.when(s == 0)
        def _():
            for d in range(2):
                out[piece(d, s, j), :] = own_and_sibling(d, s, j).astype(BF16)

        @pl.when(s > 0)
        def _():
            combine(s, j)

        for d in range(2):
            rs_copy(d, s, j).start()

    def step(i, _):
        for k in range(4):
            x_copy(i, k).wait()

        @pl.when(i > 0)
        def _():
            d2d_copy(i - 1).wait_recv()

        def gate_up(j, _):
            @pl.when(i == 0)
            def _():
                w_copy(0, j).wait()
                w_copy(1, j).wait()

            @pl.when(i > 0)
            def _():
                comm(i - 1, j)

            n = pl.ds(pl.multiple_of(j * gu_n, gu_n), gu_n)
            gate = jnp.dot(xb[...], wg_v[:, n], preferred_element_type=F32)
            up = jnp.dot(xb[...], wu_v[:, n], preferred_element_type=F32)
            hid[:, n] = (jax.nn.silu(gate) * up).astype(BF16)
            return _

        lax.fori_loop(0, SUBS, gate_up, None)

        @pl.when(i < CHIPS - 1)
        def _():
            for k in range(4):
                x_copy(i + 1, k).start()

        @pl.when(i == 0)
        def _():
            wd_copy().wait()

        @pl.when(i > 0)
        def _():
            d2d_copy(i - 1).wait_send()

        dn_n = 512

        def down(j, _):
            n = pl.ds(pl.multiple_of(j * dn_n, dn_n), dn_n)
            term = jnp.dot(hid[...], wd_v[:, n], preferred_element_type=F32)
            acc[:, n] = term[:half]
            theirs[:, n] = term[half:].astype(BF16)
            return _

        lax.fori_loop(0, cols // dn_n, down, None)
        d2d_copy(i).start()
        return _

    lax.fori_loop(0, CHIPS, step, None)

    last = CHIPS - 1
    d2d_copy(last).wait()

    def finish(j, _):
        combine(last, j)
        for d in range(2):
            ag_copy(d, 0, j).start()
            pair_copy(d, 0, j, core).start()
        return _

    lax.fori_loop(0, SUBS, finish, None)

    def gather(t, _):
        def body(j, _):
            for d in range(2):
                r = piece(d, t + CHIPS, j)
                remote(out.at[r, :], out.at[r, :], ag_send.at[d, t, j], ag_recv.at[d, t, j],
                       ring[d]).wait_recv()

                @pl.when(t < CHIPS - 2)
                def _():
                    ag_copy(d, t + 1, j).start()

                pair_copy(d, t + 1, j, core).start()
            return _

        return lax.fori_loop(0, SUBS, body, _)

    lax.fori_loop(0, CHIPS - 1, gather, None)

    def drain(t, _):
        def body(j, _):
            for d in range(2):
                @pl.when(t < CHIPS - 1)
                def _():
                    ag_copy(d, t, j).wait_send()

                pair_copy(d, t, j, core).wait_send()
                pair_copy(d, t, j, 1 - core).wait_recv()
            return _

        return lax.fori_loop(0, SUBS, body, _)

    lax.fori_loop(0, CHIPS, drain, None)


def copy_out_kernel(parts, src, dst, sem):
    n = src.shape[0] // parts
    copies = [
        pltpu.make_async_copy(src.at[pl.ds(k * n, n), :], dst.at[pl.ds(k * n, n), :], sem.at[k])
        for k in range(parts)
    ]
    for copy in copies:
        copy.start()
    for copy in copies:
        copy.wait()


def mlp(x, w_gate, w_up, w_down):
    rows, depth = x.shape
    ff = w_gate.shape[1]
    cols = w_down.shape[1]
    block = rows // CHIPS
    half = block // 2
    dma = pltpu.SemaphoreType.DMA
    any_spec = pl.BlockSpec(memory_space=pl.ANY)
    flops = 6 * rows * depth * ff
    y = pl.pallas_call(
        block_kernel,
        out_shape=pltpu.VMEM((rows, cols), BF16),
        in_specs=[any_spec] * 4,
        out_specs=pl.BlockSpec(memory_space=pltpu.VMEM),
        scratch_shapes=[
            pltpu.VMEM((depth, ff), BF16),
            pltpu.VMEM((depth, ff), BF16),
            pltpu.VMEM((ff, cols), BF16),
            pltpu.VMEM((block, depth), BF16),
            pltpu.VMEM((half, cols), F32),
            pltpu.VMEM((half, cols), BF16),
            pltpu.VMEM((2, half, cols), BF16),
            pltpu.VMEM((block, ff), BF16),
            dma((3, SUBS)),
            dma((4,)),
            dma((1,)),
            dma((2,)),
            dma((2, CHIPS - 1, SUBS)),
            dma((2, CHIPS - 1, SUBS)),
            dma((2, CHIPS - 1, SUBS)),
            dma((2, CHIPS - 1, SUBS)),
            dma((2, CHIPS, SUBS)),
            dma((2, CHIPS, SUBS)),
        ],
        compiler_params=pltpu.CompilerParams(
            collective_id=0, has_side_effects=True, vmem_limit_bytes=43 * 2**20),
        cost_estimate=pl.CostEstimate(
            flops=flops, bytes_accessed=2 * (rows * depth + 3 * depth * ff), transcendentals=rows * ff),
        name="mlp_ring",
    )(x, w_gate, w_up, w_down)
    parts = 16
    return pl.pallas_call(
        functools.partial(copy_out_kernel, parts),
        out_shape=jax.ShapeDtypeStruct((rows, cols), BF16),
        in_specs=[pl.BlockSpec(memory_space=pltpu.VMEM)],
        out_specs=any_spec,
        scratch_shapes=[dma((parts,))],
        compiler_params=pltpu.CompilerParams(vmem_limit_bytes=2**20),
        name="copy_out",
    )(y)


def solution(mesh):
    return jax.shard_map(
        mlp,
        mesh=mesh,
        in_specs=(P("dp", None), P(None, "tp"), P(None, "tp"), P("tp", None)),
        out_specs=P("dp", None),
        check_vma=False,
    )
```

```python
import functools

import jax
import jax.numpy as jnp
from jax import lax
from jax.experimental import pallas as pl
from jax.experimental.pallas import tpu as pltpu
from jax.sharding import PartitionSpec as P

MESH = pl.DeviceIdType.MESH
F32 = jnp.float32
BF16 = jnp.bfloat16

ROUNDS = 25
TREES = (
    (2, (2, 0, -1, 2, 2, 4, 4, 6), (15, 6, -1, 17, 18, 9, 17, 5), (19, 20, -1, 22, 19, 21, 20, 21)),
    (0, (-1, 0, 4, 1, 6, 3, 7, 5), (-1, 7, 0, 6, 1, 4, 2, 3), (-1, 8, 23, 9, 22, 10, 15, 11)),
    (0, (-1, 0, 3, 1, 2, 3, 7, 5), (-1, 9, 3, 7, 1, 6, 4, 5), (-1, 10, 20, 19, 24, 21, 23, 22)),
    (2, (2, 3, -1, 2, 6, 3, 7, 5), (12, 11, -1, 12, 2, 5, 3, 4), (13, 14, -1, 13, 20, 14, 16, 15)),
    (0, (-1, 3, 0, 2, 6, 3, 7, 5), (-1, 1, 5, 4, 0, 3, 1, 2), (-1, 8, 6, 7, 21, 8, 11, 9)),
    (0, (-1, 3, 0, 2, 2, 4, 4, 6), (-1, 10, 12, 11, 11, 2, 8, 0), (-1, 24, 13, 15, 15, 16, 16, 17)),
    (0, (-1, 0, 0, 2, 2, 3, 4, 5), (-1, 14, 10, 8, 9, 7, 7, 0), (-1, 18, 18, 19, 22, 20, 23, 21)),
    (2, (2, 0, -1, 2, 2, 4, 4, 6), (16, 12, -1, 14, 16, 10, 14, 13), (17, 19, -1, 18, 17, 23, 18, 22)),
)
NODES = range(8)
SUBS = 2
SLOT = 2


def outer(v):
    return v // 2 in (0, 3)


def children(b, v):
    _, parent, up, _ = TREES[b]
    return sorted((c for c in NODES if parent[c] == v), key=lambda c: up[c])


def use_round(b, v):
    root, _, up, _ = TREES[b]
    return max(up[c] for c in children(b, v)) + 1 if v == root else up[v]


def plan_steps(is_outer):
    items = sorted((use_round(b, v), b, v) for b in range(len(TREES)) for v in NODES if outer(v) == is_outer)
    steps = {}
    for use, b, v in reversed(items):
        if not steps or len(steps[min(steps)]) == SLOT:
            step = min([use, *(s - 1 for s in steps)])
        else:
            step = min(use, min(steps))
        assert step == use
        steps.setdefault(step, []).append((b, v))
    assert min(steps) >= 0
    return {s: sorted(units) for s, units in steps.items()}


def port_of(v, w):
    if v // 2 == w // 2:
        return 0
    return 1 if outer(v) or outer(w) else 2


STEPS = {o: plan_steps(o) for o in (True, False)}
EXTRA = {}
for _o in (True, False):
    _found = [(b, v, c) for b in range(len(TREES)) for v in NODES if outer(v) == _o for c in children(b, v)[1:]]
    EXTRA.update({key: k for k, key in enumerate(_found)})
N_EXTRA = max(EXTRA.values()) + 1
SENDS = {(o, e): [] for o in (True, False) for e in range(3)}
for _b, (_root, _parent, _up, _down) in enumerate(TREES):
    for _v in NODES:
        if _v != _root:
            SENDS[outer(_v), port_of(_v, _parent[_v])].append(_up[_v])
            SENDS[outer(_parent[_v]), port_of(_v, _parent[_v])].append(_down[_v])
assert all(len(set(rounds)) == len(rounds) for rounds in SENDS.values())


def select(index, values):
    out = jnp.int32(values[0])
    for k, value in enumerate(values):
        if k:
            out = jnp.where(index == k, jnp.int32(value), out)
    return out


def block_kernel(x, wg, wu, wd, out, wg_v, wu_v, wd_v, xb, acc, theirs, d2d, hid, stage, extra,
                 w_sem, x_sem, d2d_send, d2d_recv, send_sem, rs_recv, extra_recv, ag_recv, pair_send, pair_recv):
    rows = x.shape[0]
    cols = wd.shape[1]
    n_units = 4 * len(TREES)
    unit = rows // n_units
    half = unit // 2
    sub = half // SUBS

    tp = lax.axis_index("tp")
    core = tp % 2
    z = (tp // 2) % 4
    y = tp // 8
    far = z // 2
    nz = z + far * (3 - 2 * z)
    is_outer = nz == 0
    is_inner = nz == 1
    toward = 1 - 2 * far

    def device(yy, zz):
        return (yy * 4 + zz) * 2 + core

    sibling = tp + 1 - 2 * core
    ports = {
        True: (device(1 - y, z), device(y, z + toward)),
        False: (device(1 - y, z), device(y, z - toward), device(y, z + toward)),
    }

    def code(b, v):
        return 4 * b + 2 * (v % 2) + (v // 2) // 2

    def image(q):
        return 4 * (q // 4) + 2 * (((q // 2) % 2 + y) % 2) + (q % 2 + far) % 2

    def piece(u, j, c=None):
        return pl.ds(pl.multiple_of(u * unit + (core if c is None else c) * half + sub * j, sub), sub)

    def remote(src, dst, send, recv, to):
        return pltpu.make_async_remote_copy(
            src_ref=src, dst_ref=dst, send_sem=send, recv_sem=recv,
            device_id={"tp": to}, device_id_type=MESH)

    def landing(b, v, c, u, j):
        if children(b, v)[0] == c:
            return out.at[piece(u, j), :], rs_recv.at[u, j]
        k = EXTRA[b, v, c]
        return extra.at[k, pl.ds(pl.multiple_of(sub * j, sub), sub), :], extra_recv.at[k, j]

    def pair_copy(u, j, c=None):
        r = piece(u, j, c)
        return remote(out.at[r, :], out.at[r, :], pair_send.at[u, j], pair_recv.at[u, j], sibling)

    def d2d_copy(s):
        return remote(theirs, d2d.at[s % 2], d2d_send.at[0], d2d_recv.at[s % 2], sibling)

    n_steps = jnp.where(is_outer, max(STEPS[True]) + 1, max(STEPS[False]) + 1)
    most = max(max(STEPS[True]), max(STEPS[False])) + 1

    def step_units(s):
        picked = []
        for k in range(SLOT):
            q = {}
            for o in (True, False):
                table = []
                for i in range(most):
                    items = STEPS[o].get(i, [(0, 0 if o else 2)])
                    b, v = items[min(k, len(items) - 1)]
                    table.append(code(b, v))
                q[o] = select(s, table)
            picked.append(image(jnp.where(is_outer, q[True], q[False])))
        return picked

    def x_copies(s):
        copies = []
        units = step_units(s)
        for other in range(2):
            c = core + other * (1 - 2 * core)
            for k in range(SLOT):
                n = other * SLOT + k
                start = pl.multiple_of(units[k] * unit + c * half, half)
                copies.append(pltpu.make_async_copy(
                    x.at[pl.ds(start, half), :], xb.at[pl.ds(n * half, half), :], x_sem.at[n]))
        return copies

    w_copies = [
        pltpu.make_async_copy(wg, wg_v, w_sem.at[0]),
        pltpu.make_async_copy(wu, wu_v, w_sem.at[1]),
        pltpu.make_async_copy(wd, wd_v, w_sem.at[2]),
    ]
    for copy in x_copies(jnp.int32(0)) + w_copies:
        copy.start()

    barrier = pltpu.get_barrier_semaphore()
    for o, here in ((True, is_outer), (False, is_inner)):
        @pl.when(here)
        def _(o=o):
            for to in (*ports[o], sibling):
                pl.semaphore_signal(barrier, inc=1, device_id={"tp": to}, device_id_type=MESH)
            pl.semaphore_wait(barrier, len(ports[o]) + 1)

    def send(o, e, r, j, src, dst, recv):
        remote(src, dst, send_sem.at[e, r % 2, j], recv, ports[o][e]).start()

    def free_slot(o, e, r, j):
        if any(k < r and (r - k) % 2 == 0 for k in SENDS[o, e]):
            slot = stage.at[e, r % 2, j]
            remote(slot, slot, send_sem.at[e, r % 2, j], ag_recv.at[0, 0], ports[o][e]).wait_send()

    def total(o, b, v, u, j, store):
        use = use_round(b, v)
        k = STEPS[o][use].index((b, v))
        r = pl.ds(pl.multiple_of(k * half + sub * j, sub), sub)
        places = []
        for c in children(b, v):
            ref, sem = landing(b, v, c, u, j)
            remote(ref, ref, send_sem.at[0, 0, 0], sem, sibling).wait_recv()
            places.append(ref)
        value = acc[r, :] + d2d[use % 2, r, :].astype(F32)
        for ref in places:
            value = value + ref[...].astype(F32)
        store[...] = value.astype(BF16)

    def comm(o, r, j):
        nodes = [(b, v) for b in range(len(TREES)) for v in NODES if outer(v) == o]
        for b, v in nodes:
            root, parent, up, down = TREES[b]
            if v != root and down[v] == r - 1:
                u = image(code(b, v))
                mine = out.at[piece(u, j), :]
                remote(mine, mine, send_sem.at[0, 0, 0], ag_recv.at[u, j], sibling).wait_recv()
                pair_copy(u, j).start()
        for b, v in nodes:
            if v == TREES[b][0] and use_round(b, v) == r:
                u = image(code(b, v))
                total(o, b, v, u, j, out.at[piece(u, j), :])
                pair_copy(u, j).start()
        for b, v in nodes:
            root, parent, up, down = TREES[b]
            for w in children(b, v):
                if down[w] == r:
                    u = image(code(b, v))
                    e = port_of(v, w)
                    free_slot(o, e, r, j)
                    r_out = out.at[piece(u, j), :]
                    send(o, e, r, j, r_out, r_out, ag_recv.at[u, j])
            if v != root and up[v] == r:
                u = image(code(b, v))
                e = port_of(v, parent[v])
                free_slot(o, e, r, j)
                slot = stage.at[e, r % 2, j]
                total(o, b, v, u, j, slot)
                send(o, e, r, j, slot, *landing(b, parent[v], v, u, j))

    def gate_up(s):
        for copy in x_copies(s):
            copy.wait()

        @pl.when(s == 0)
        def _():
            w_copies[0].wait()
            w_copies[1].wait()

        gate = jnp.dot(xb[...], wg_v[...], preferred_element_type=F32)
        up = jnp.dot(xb[...], wu_v[...], preferred_element_type=F32)
        hid[...] = (jax.nn.silu(gate) * up).astype(BF16)

        @pl.when(s + 1 < n_steps)
        def _():
            for copy in x_copies(s + 1):
                copy.start()

    def down_proj(s):
        @pl.when(s == 0)
        def _():
            w_copies[2].wait()

        @pl.when(s > 0)
        def _():
            d2d_copy(s - 1).wait_send()

        n_cols = cols // 2

        def part(k, carry):
            n = pl.ds(pl.multiple_of(k * n_cols, n_cols), n_cols)
            term = jnp.dot(hid[...], wd_v[:, n], preferred_element_type=F32)
            acc[:, n] = term[:SLOT * half]
            theirs[:, n] = term[SLOT * half:].astype(BF16)
            return carry

        lax.fori_loop(0, cols // n_cols, part, None)
        d2d_copy(s).start()

    def round_(i, carry):
        r = i - 1
        s = r + 1

        @pl.when((r >= 0) & (r < n_steps))
        def _():
            d2d_copy(r).wait_recv()

        def body(j, carry):
            for o, here in ((True, is_outer), (False, is_inner)):
                @pl.when(here)
                def _(o=o):
                    for k in range(ROUNDS + 1):
                        @pl.when(r == k)
                        def _(k=k):
                            comm(o, k, j)

            @pl.when((s < n_steps) & (j == 0))
            def _():
                gate_up(s)

            @pl.when((s < n_steps) & (j == SUBS - 1))
            def _():
                down_proj(s)

            return carry

        return lax.fori_loop(0, SUBS, body, carry)

    lax.fori_loop(0, ROUNDS + 2, round_, None)

    for o, here in ((True, is_outer), (False, is_inner)):
        @pl.when(here)
        def _(o=o):
            for e in range(len(ports[o])):
                for parity in sorted({r % 2 for r in SENDS[o, e]}):
                    for j in range(SUBS):
                        slot = stage.at[e, parity, j]
                        remote(slot, slot, send_sem.at[e, parity, j], ag_recv.at[0, 0], ports[o][e]).wait_send()

    d2d_copy(n_steps - 1).wait_send()

    def drain(u, carry):
        for j in range(SUBS):
            pair_copy(u, j).wait_send()
            pair_copy(u, j, 1 - core).wait_recv()
        return carry

    lax.fori_loop(0, n_units, drain, None)


def copy_out_kernel(parts, src, dst, sem):
    n = src.shape[0] // parts
    copies = [
        pltpu.make_async_copy(src.at[pl.ds(k * n, n), :], dst.at[pl.ds(k * n, n), :], sem.at[k])
        for k in range(parts)
    ]
    for copy in copies:
        copy.start()
    for copy in copies:
        copy.wait()


def mlp(x, w_gate, w_up, w_down):
    rows, depth = x.shape
    ff = w_gate.shape[1]
    cols = w_down.shape[1]
    n_units = 4 * len(TREES)
    half = rows // n_units // 2
    sub = half // SUBS
    dma = pltpu.SemaphoreType.DMA
    any_spec = pl.BlockSpec(memory_space=pl.ANY)
    y = pl.pallas_call(
        block_kernel,
        out_shape=pltpu.VMEM((rows, cols), BF16),
        in_specs=[any_spec] * 4,
        out_specs=pl.BlockSpec(memory_space=pltpu.VMEM),
        scratch_shapes=[
            pltpu.VMEM((depth, ff), BF16),
            pltpu.VMEM((depth, ff), BF16),
            pltpu.VMEM((ff, cols), BF16),
            pltpu.VMEM((2 * SLOT * half, depth), BF16),
            pltpu.VMEM((SLOT * half, cols), F32),
            pltpu.VMEM((SLOT * half, cols), BF16),
            pltpu.VMEM((2, SLOT * half, cols), BF16),
            pltpu.VMEM((2 * SLOT * half, ff), BF16),
            pltpu.VMEM((3, 2, SUBS, sub, cols), BF16),
            pltpu.VMEM((N_EXTRA, half, cols), BF16),
            dma((3,)),
            dma((2 * SLOT,)),
            dma((1,)),
            dma((2,)),
            dma((3, 2, SUBS)),
            dma((n_units, SUBS)),
            dma((N_EXTRA, SUBS)),
            dma((n_units, SUBS)),
            dma((n_units, SUBS)),
            dma((n_units, SUBS)),
        ],
        compiler_params=pltpu.CompilerParams(
            collective_id=0, has_side_effects=True, vmem_limit_bytes=43 * 2**20),
        cost_estimate=pl.CostEstimate(
            flops=6 * rows * depth * ff, bytes_accessed=2 * (rows * depth + 3 * depth * ff),
            transcendentals=rows * ff),
        name="mlp_trees",
    )(x, w_gate, w_up, w_down)
    parts = 16
    return pl.pallas_call(
        functools.partial(copy_out_kernel, parts),
        out_shape=jax.ShapeDtypeStruct((rows, cols), BF16),
        in_specs=[pl.BlockSpec(memory_space=pltpu.VMEM)],
        out_specs=any_spec,
        scratch_shapes=[dma((parts,))],
        compiler_params=pltpu.CompilerParams(vmem_limit_bytes=2**20),
        name="copy_out",
    )(y)


def solution(mesh):
    return jax.shard_map(
        mlp,
        mesh=mesh,
        in_specs=(P("dp", None), P(None, "tp"), P(None, "tp"), P("tp", None)),
        out_specs=P("dp", None),
        check_vma=False,
    )
```

```python
import functools

import jax
import jax.numpy as jnp
from jax import lax
from jax.experimental import pallas as pl
from jax.experimental.pallas import tpu as pltpu
from jax.sharding import PartitionSpec as P

MESH = pl.DeviceIdType.MESH
F32 = jnp.float32
BF16 = jnp.bfloat16

ROUNDS = 24
TREES = (
    (0, (-1, 0, 0, 2, 2, 4, 4, 6), (-1, 9, 13, 9, 12, 8, 11, 4), (-1, 15, 14, 19, 15, 18, 16, 17)),
    (0, (-1, 3, 0, 5, 2, 4, 4, 5), (-1, 8, 14, 10, 13, 11, 12, 10), (-1, 23, 15, 19, 16, 17, 17, 20)),
    (0, (-1, 0, 0, 2, 2, 4, 4, 6), (-1, 16, 19, 14, 18, 12, 17, 1), (-1, 21, 20, 21, 21, 23, 22, 23)),
    (0, (-1, 3, 0, 2, 2, 3, 4, 5), (-1, 1, 4, 3, 3, 2, 2, 0), (-1, 8, 5, 6, 6, 9, 7, 11)),
    (0, (-1, 0, 3, 1, 6, 3, 7, 5), (-1, 10, 7, 9, 0, 7, 5, 6), (-1, 12, 15, 13, 21, 14, 18, 15)),
    (0, (-1, 0, 0, 2, 2, 4, 4, 6), (-1, 13, 18, 10, 17, 16, 16, 0), (-1, 20, 19, 20, 20, 22, 21, 22)),
    (0, (-1, 0, 0, 5, 2, 7, 4, 6), (-1, 6, 5, 0, 4, 1, 3, 2), (-1, 14, 7, 23, 8, 18, 10, 11)),
    (0, (-1, 0, 3, 1, 6, 3, 7, 5), (-1, 7, 1, 6, 2, 5, 3, 4), (-1, 8, 13, 9, 23, 11, 19, 12)),
)
NODES = range(8)
GROUP = 5
SUBS = 2
SLOT = 2
AHEAD = 3
PIECES = 4


def outer(v):
    return v // 2 in (0, 3)


def children(b, v):
    _, parent, up, _ = TREES[b]
    return sorted((c for c in NODES if parent[c] == v), key=lambda c: up[c])


def use_round(b, v):
    root, _, up, _ = TREES[b]
    return max(up[c] for c in children(b, v)) + 1 if v == root else up[v]


def plan_steps(is_outer):
    items = sorted((use_round(b, v), b, v) for b in range(len(TREES)) for v in NODES if outer(v) == is_outer)
    steps = {}
    for use, b, v in reversed(items):
        if not steps or len(steps[min(steps)]) == SLOT:
            step = min([use, *(s - 1 for s in steps)])
        else:
            step = min(use, min(steps))
        assert step == use
        steps.setdefault(step, []).append((b, v))
    assert min(steps) >= 0
    return {s: sorted(units) for s, units in steps.items()}


def port_of(v, w):
    if v // 2 == w // 2:
        return 0
    return 1 if outer(v) or outer(w) else 2


STEPS = {o: plan_steps(o) for o in (True, False)}
EXTRA = {}
for _o in (True, False):
    _found = [(b, v, c) for b in range(len(TREES)) for v in NODES if outer(v) == _o for c in children(b, v)[1:]]
    EXTRA.update({key: k for k, key in enumerate(_found)})
N_EXTRA = max(EXTRA.values()) + 1
SENDS = {(o, e): [] for o in (True, False) for e in range(3)}
for _b, (_root, _parent, _up, _down) in enumerate(TREES):
    for _v in NODES:
        if _v != _root:
            SENDS[outer(_v), port_of(_v, _parent[_v])].append(_up[_v])
            SENDS[outer(_parent[_v]), port_of(_v, _parent[_v])].append(_down[_v])
assert all(len(set(rounds)) == len(rounds) for rounds in SENDS.values())


def select(index, values):
    out = jnp.int32(values[0])
    for k, value in enumerate(values):
        if k:
            out = jnp.where(index == k, jnp.int32(value), out)
    return out


def block_kernel(x, wg, wu, wd, out, wg_v, wu_v, wd_v, xb, acc, theirs, d2d, hid, stage, extra,
                 w_sem, x_sem, d2d_send, d2d_recv, send_sem, rs_recv, extra_recv, ag_recv, pair_send, pair_recv):
    rows = x.shape[0]
    cols = wd.shape[1]
    n_units = 4 * len(TREES)
    unit = rows // n_units
    half = unit // 2
    sub = half // SUBS

    tp = lax.axis_index("tp")
    core = tp % 2
    z = (tp // 2) % 4
    y = tp // 8
    far = z // 2
    nz = z + far * (3 - 2 * z)
    is_outer = nz == 0
    is_inner = nz == 1
    toward = 1 - 2 * far

    def device(yy, zz):
        return (yy * 4 + zz) * 2 + core

    sibling = tp + 1 - 2 * core
    ports = {
        True: (device(1 - y, z), device(y, z + toward)),
        False: (device(1 - y, z), device(y, z - toward), device(y, z + toward)),
    }

    def code(b, v):
        return 4 * b + 2 * (v % 2) + (v // 2) // 2

    def image(q):
        return 4 * (q // 4) + 2 * (((q // 2) % 2 + y) % 2) + (q % 2 + far) % 2

    def piece(u, j, c=None):
        return pl.ds(pl.multiple_of(u * unit + (core if c is None else c) * half + sub * j, sub), sub)

    def remote(src, dst, send, recv, to):
        return pltpu.make_async_remote_copy(
            src_ref=src, dst_ref=dst, send_sem=send, recv_sem=recv,
            device_id={"tp": to}, device_id_type=MESH)

    def landing(b, v, c, u, j):
        if children(b, v)[0] == c:
            return out.at[piece(u, j), :], rs_recv.at[u, j]
        k = EXTRA[b, v, c]
        return extra.at[k, pl.ds(pl.multiple_of(sub * j, sub), sub), :], extra_recv.at[k, j]

    def pair_copy(u, j, c=None):
        r = piece(u, j, c)
        return remote(out.at[r, :], out.at[r, :], pair_send.at[u, j], pair_recv.at[u, j], sibling)

    def d2d_copy(s):
        return remote(theirs, d2d.at[s % 2], d2d_send.at[0], d2d_recv.at[s % 2], sibling)

    n_steps = jnp.where(is_outer, max(STEPS[True]) + 1, max(STEPS[False]) + 1)
    most = max(max(STEPS[True]), max(STEPS[False])) + 1

    def step_units(s):
        picked = []
        for k in range(SLOT):
            q = {}
            for o in (True, False):
                table = []
                for i in range(most):
                    items = STEPS[o].get(i, [(0, 0 if o else 2)])
                    b, v = items[min(k, len(items) - 1)]
                    table.append(code(b, v))
                q[o] = select(s, table)
            picked.append(image(jnp.where(is_outer, q[True], q[False])))
        return picked

    def x_copy(start, n):
        return pltpu.make_async_copy(
            x.at[pl.ds(start, half), :], xb.at[pl.ds(n * half, half), :], x_sem.at[n])

    def x_copies(s):
        units = step_units(s)
        copies = []
        for n in range(2 * SLOT):
            c = core if n < SLOT else 1 - core
            copies.append(x_copy(pl.multiple_of(units[n % SLOT] * unit + c * half, half), n))
        return copies

    g_cols = wg.shape[1] // PIECES
    d_cols = cols // PIECES

    def w_copy(i, k):
        width = d_cols if i == 2 else g_cols
        n = pl.ds(pl.multiple_of(k * width, width), width)
        src, dst = ((wg, wg_v), (wu, wu_v), (wd, wd_v))[i]
        return pltpu.make_async_copy(src.at[:, n], dst.at[:, n], w_sem.at[i, k])

    def load(k):
        @pl.when(k < PIECES)
        def _():
            w_copy(0, k).start()
            w_copy(1, k).start()

        @pl.when((k >= PIECES) & (2 * (k - PIECES) < PIECES))
        def _():
            w_copy(2, 2 * (k - PIECES)).start()
            w_copy(2, 2 * (k - PIECES) + 1).start()

    for copy in x_copies(jnp.int32(0)):
        copy.start()
    for k in range(AHEAD):
        load(jnp.int32(k))

    barrier = pltpu.get_barrier_semaphore()
    for o, here in ((True, is_outer), (False, is_inner)):
        @pl.when(here)
        def _(o=o):
            for to in (*ports[o], sibling):
                pl.semaphore_signal(barrier, inc=1, device_id={"tp": to}, device_id_type=MESH)
            pl.semaphore_wait(barrier, len(ports[o]) + 1)

    def send(o, e, r, j, src, dst, recv):
        remote(src, dst, send_sem.at[e, r % 2, j], recv, ports[o][e]).start()

    def free_slot(o, e, r, j):
        if any(k < r and (r - k) % 2 == 0 for k in SENDS[o, e]):
            slot = stage.at[e, r % 2, j]
            remote(slot, slot, send_sem.at[e, r % 2, j], ag_recv.at[0, 0], ports[o][e]).wait_send()

    def total(o, b, v, u, j, store):
        use = use_round(b, v)
        k = STEPS[o][use].index((b, v))
        r = pl.ds(pl.multiple_of(k * half + sub * j, sub), sub)
        places = []
        for c in children(b, v):
            ref, sem = landing(b, v, c, u, j)
            remote(ref, ref, send_sem.at[0, 0, 0], sem, sibling).wait_recv()
            places.append(ref)
        value = acc[r, :] + d2d[use % 2, r, :].astype(F32)
        for ref in places:
            value = value + ref[...].astype(F32)
        store[...] = value.astype(BF16)

    def comm(o, r, j):
        nodes = [(b, v) for b in range(len(TREES)) for v in NODES if outer(v) == o]
        for b, v in nodes:
            root, parent, up, down = TREES[b]
            if v != root and down[v] == r - 1:
                u = image(code(b, v))
                mine = out.at[piece(u, j), :]
                remote(mine, mine, send_sem.at[0, 0, 0], ag_recv.at[u, j], sibling).wait_recv()
                pair_copy(u, j).start()
        for b, v in nodes:
            if v == TREES[b][0] and use_round(b, v) == r:
                u = image(code(b, v))
                total(o, b, v, u, j, out.at[piece(u, j), :])
                pair_copy(u, j).start()
        for b, v in nodes:
            root, parent, up, down = TREES[b]
            for w in children(b, v):
                if down[w] == r:
                    u = image(code(b, v))
                    e = port_of(v, w)
                    free_slot(o, e, r, j)
                    r_out = out.at[piece(u, j), :]
                    send(o, e, r, j, r_out, r_out, ag_recv.at[u, j])
            if v != root and up[v] == r:
                u = image(code(b, v))
                e = port_of(v, parent[v])
                free_slot(o, e, r, j)
                slot = stage.at[e, r % 2, j]
                total(o, b, v, u, j, slot)
                send(o, e, r, j, slot, *landing(b, parent[v], v, u, j))

    def gate_up(s):
        for n in range(2 * SLOT):
            x_copy(0, n).wait()

        def hidden(n):
            gate = jnp.dot(xb[...], wg_v[:, n], preferred_element_type=F32)
            up = jnp.dot(xb[...], wu_v[:, n], preferred_element_type=F32)
            hid[:, n] = (jax.nn.silu(gate) * up).astype(BF16)

        @pl.when(s == 0)
        def _():
            def part(k, carry):
                w_copy(0, k).wait()
                w_copy(1, k).wait()
                load(k + AHEAD)
                hidden(pl.ds(pl.multiple_of(k * g_cols, g_cols), g_cols))
                return carry

            lax.fori_loop(0, PIECES, part, None)

        @pl.when(s > 0)
        def _():
            hidden(slice(None))

        @pl.when(s + 1 < n_steps)
        def _():
            for copy in x_copies(s + 1):
                copy.start()

    def down_proj(s):
        def term(n):
            value = jnp.dot(hid[...], wd_v[:, n], preferred_element_type=F32)
            acc[:, n] = value[:SLOT * half]
            theirs[:, n] = value[SLOT * half:].astype(BF16)

        @pl.when(s == 0)
        def _():
            def part(k, carry):
                w_copy(2, k).wait()
                term(pl.ds(pl.multiple_of(k * d_cols, d_cols), d_cols))
                return carry

            lax.fori_loop(0, PIECES, part, None)

        @pl.when(s > 0)
        def _():
            d2d_copy(s - 1).wait_send()
            n_cols = cols

            def part(k, carry):
                term(pl.ds(pl.multiple_of(k * n_cols, n_cols), n_cols))
                return carry

            lax.fori_loop(0, cols // n_cols, part, None)

        d2d_copy(s).start()

    def round_(i, carry):
        r = i - 1
        s = r + 1

        @pl.when((r >= 0) & (r < n_steps))
        def _():
            d2d_copy(r).wait_recv()

        def body(j, carry):
            for o, here in ((True, is_outer), (False, is_inner)):
                @pl.when(here)
                def _(o=o):
                    for first in range(0, ROUNDS + 1, GROUP):
                        @pl.when((r >= first) & (r < first + GROUP))
                        def _(first=first):
                            for k in range(first, min(first + GROUP, ROUNDS + 1)):
                                @pl.when(r == k)
                                def _(k=k):
                                    comm(o, k, j)

            @pl.when((s < n_steps) & (j == 0))
            def _():
                gate_up(s)

            @pl.when((s < n_steps) & (j == SUBS - 1))
            def _():
                down_proj(s)

            return carry

        return lax.fori_loop(0, SUBS, body, carry)

    lax.fori_loop(0, ROUNDS + 2, round_, None)

    for o, here in ((True, is_outer), (False, is_inner)):
        @pl.when(here)
        def _(o=o):
            for e in range(len(ports[o])):
                for parity in sorted({r % 2 for r in SENDS[o, e]}):
                    for j in range(SUBS):
                        slot = stage.at[e, parity, j]
                        remote(slot, slot, send_sem.at[e, parity, j], ag_recv.at[0, 0], ports[o][e]).wait_send()

    d2d_copy(n_steps - 1).wait_send()

    def drain(u, carry):
        for j in range(SUBS):
            pair_copy(u, j).wait_send()
            pair_copy(u, j, 1 - core).wait_recv()
        return carry

    lax.fori_loop(0, n_units, drain, None)


def copy_out_kernel(parts, src, dst, sem):
    n = src.shape[0] // parts
    copies = [
        pltpu.make_async_copy(src.at[pl.ds(k * n, n), :], dst.at[pl.ds(k * n, n), :], sem.at[k])
        for k in range(parts)
    ]
    for copy in copies:
        copy.start()
    for copy in copies:
        copy.wait()


def mlp(x, w_gate, w_up, w_down):
    rows, depth = x.shape
    ff = w_gate.shape[1]
    cols = w_down.shape[1]
    n_units = 4 * len(TREES)
    half = rows // n_units // 2
    sub = half // SUBS
    dma = pltpu.SemaphoreType.DMA
    any_spec = pl.BlockSpec(memory_space=pl.ANY)
    y = pl.pallas_call(
        block_kernel,
        out_shape=pltpu.VMEM((rows, cols), BF16),
        in_specs=[any_spec] * 4,
        out_specs=pl.BlockSpec(memory_space=pltpu.VMEM),
        scratch_shapes=[
            pltpu.VMEM((depth, ff), BF16),
            pltpu.VMEM((depth, ff), BF16),
            pltpu.VMEM((ff, cols), BF16),
            pltpu.VMEM((2 * SLOT * half, depth), BF16),
            pltpu.VMEM((SLOT * half, cols), F32),
            pltpu.VMEM((SLOT * half, cols), BF16),
            pltpu.VMEM((2, SLOT * half, cols), BF16),
            pltpu.VMEM((2 * SLOT * half, ff), BF16),
            pltpu.VMEM((3, 2, SUBS, sub, cols), BF16),
            pltpu.VMEM((N_EXTRA, half, cols), BF16),
            dma((3, PIECES)),
            dma((2 * SLOT,)),
            dma((1,)),
            dma((2,)),
            dma((3, 2, SUBS)),
            dma((n_units, SUBS)),
            dma((N_EXTRA, SUBS)),
            dma((n_units, SUBS)),
            dma((n_units, SUBS)),
            dma((n_units, SUBS)),
        ],
        compiler_params=pltpu.CompilerParams(
            collective_id=0, has_side_effects=True, vmem_limit_bytes=43 * 2**20),
        cost_estimate=pl.CostEstimate(
            flops=6 * rows * depth * ff, bytes_accessed=2 * (rows * depth + 3 * depth * ff),
            transcendentals=rows * ff),
        name="mlp_trees",
    )(x, w_gate, w_up, w_down)
    parts = 8
    return pl.pallas_call(
        functools.partial(copy_out_kernel, parts),
        out_shape=jax.ShapeDtypeStruct((rows, cols), BF16),
        in_specs=[pl.BlockSpec(memory_space=pltpu.VMEM)],
        out_specs=any_spec,
        scratch_shapes=[dma((parts,))],
        compiler_params=pltpu.CompilerParams(vmem_limit_bytes=2**20),
        name="copy_out",
    )(y)


def solution(mesh):
    return jax.shard_map(
        mlp,
        mesh=mesh,
        in_specs=(P("dp", None), P(None, "tp"), P(None, "tp"), P("tp", None)),
        out_specs=P("dp", None),
        check_vma=False,
    )
```

```python
import functools

import jax
import jax.numpy as jnp
from jax import lax
from jax.experimental import pallas as pl
from jax.experimental.pallas import tpu as pltpu
from jax.sharding import PartitionSpec as P

MESH = pl.DeviceIdType.MESH
F32 = jnp.float32
BF16 = jnp.bfloat16

ROUNDS = 24
TREES = (
    (0, (-1, 0, 0, 2, 2, 4, 4, 6), (-1, 9, 13, 9, 12, 8, 11, 4), (-1, 15, 14, 19, 15, 18, 16, 17)),
    (0, (-1, 3, 0, 5, 2, 4, 4, 5), (-1, 8, 14, 10, 13, 11, 12, 10), (-1, 23, 15, 19, 16, 17, 17, 20)),
    (0, (-1, 0, 0, 2, 2, 4, 4, 6), (-1, 16, 19, 14, 18, 12, 17, 1), (-1, 21, 20, 21, 21, 23, 22, 23)),
    (0, (-1, 3, 0, 2, 2, 3, 4, 5), (-1, 1, 4, 3, 3, 2, 2, 0), (-1, 8, 5, 6, 6, 9, 7, 11)),
    (0, (-1, 0, 3, 1, 6, 3, 7, 5), (-1, 10, 7, 9, 0, 7, 5, 6), (-1, 12, 15, 13, 21, 14, 18, 15)),
    (0, (-1, 0, 0, 2, 2, 4, 4, 6), (-1, 13, 18, 10, 17, 16, 16, 0), (-1, 20, 19, 20, 20, 22, 21, 22)),
    (0, (-1, 0, 0, 5, 2, 7, 4, 6), (-1, 6, 5, 0, 4, 1, 3, 2), (-1, 14, 7, 23, 8, 18, 10, 11)),
    (0, (-1, 0, 3, 1, 6, 3, 7, 5), (-1, 7, 1, 6, 2, 5, 3, 4), (-1, 8, 13, 9, 23, 11, 19, 12)),
)
NODES = range(8)
GROUP = 5
SUBS = 2
SLOT = 2
AHEAD = 3
PIECES = 4


def outer(v):
    return v // 2 in (0, 3)


def children(b, v):
    _, parent, up, _ = TREES[b]
    return sorted((c for c in NODES if parent[c] == v), key=lambda c: up[c])


def use_round(b, v):
    root, _, up, _ = TREES[b]
    return max(up[c] for c in children(b, v)) + 1 if v == root else up[v]


def plan_steps(is_outer):
    items = sorted((use_round(b, v), b, v) for b in range(len(TREES)) for v in NODES if outer(v) == is_outer)
    steps = {}
    for use, b, v in reversed(items):
        if not steps or len(steps[min(steps)]) == SLOT:
            step = min([use, *(s - 1 for s in steps)])
        else:
            step = min(use, min(steps))
        assert step == use
        steps.setdefault(step, []).append((b, v))
    assert min(steps) >= 0
    return {s: sorted(units) for s, units in steps.items()}


def port_of(v, w):
    if v // 2 == w // 2:
        return 0
    return 1 if outer(v) or outer(w) else 2


STEPS = {o: plan_steps(o) for o in (True, False)}
EXTRA = {}
for _o in (True, False):
    _found = [(b, v, c) for b in range(len(TREES)) for v in NODES if outer(v) == _o for c in children(b, v)[1:]]
    EXTRA.update({key: k for k, key in enumerate(_found)})
N_EXTRA = max(EXTRA.values()) + 1
SENDS = {(o, e): [] for o in (True, False) for e in range(3)}
for _b, (_root, _parent, _up, _down) in enumerate(TREES):
    for _v in NODES:
        if _v != _root:
            SENDS[outer(_v), port_of(_v, _parent[_v])].append(_up[_v])
            SENDS[outer(_parent[_v]), port_of(_v, _parent[_v])].append(_down[_v])
assert all(len(set(rounds)) == len(rounds) for rounds in SENDS.values())


def select(index, values):
    out = jnp.int32(values[0])
    for k, value in enumerate(values):
        if k:
            out = jnp.where(index == k, jnp.int32(value), out)
    return out


def block_kernel(x, wg, wu, wd, out, wg_v, wu_v, wd_v, xb, acc, theirs, d2d, hid, stage, extra,
                 w_sem, x_sem, first_send, first_recv, d2d_send, d2d_recv, send_sem, rs_recv, extra_recv, ag_recv, pair_send, pair_recv):
    rows = x.shape[0]
    cols = wd.shape[1]
    n_units = 4 * len(TREES)
    unit = rows // n_units
    half = unit // 2
    sub = half // SUBS

    tp = lax.axis_index("tp")
    core = tp % 2
    z = (tp // 2) % 4
    y = tp // 8
    far = z // 2
    nz = z + far * (3 - 2 * z)
    is_outer = nz == 0
    is_inner = nz == 1
    toward = 1 - 2 * far

    def device(yy, zz):
        return (yy * 4 + zz) * 2 + core

    sibling = tp + 1 - 2 * core
    ports = {
        True: (device(1 - y, z), device(y, z + toward)),
        False: (device(1 - y, z), device(y, z - toward), device(y, z + toward)),
    }

    def code(b, v):
        return 4 * b + 2 * (v % 2) + (v // 2) // 2

    def image(q):
        return 4 * (q // 4) + 2 * (((q // 2) % 2 + y) % 2) + (q % 2 + far) % 2

    def piece(u, j, c=None):
        return pl.ds(pl.multiple_of(u * unit + (core if c is None else c) * half + sub * j, sub), sub)

    def remote(src, dst, send, recv, to):
        return pltpu.make_async_remote_copy(
            src_ref=src, dst_ref=dst, send_sem=send, recv_sem=recv,
            device_id={"tp": to}, device_id_type=MESH)

    def landing(b, v, c, u, j):
        if children(b, v)[0] == c:
            return out.at[piece(u, j), :], rs_recv.at[u, j]
        k = EXTRA[b, v, c]
        return extra.at[k, pl.ds(pl.multiple_of(sub * j, sub), sub), :], extra_recv.at[k, j]

    def pair_copy(u, j, c=None):
        r = piece(u, j, c)
        return remote(out.at[r, :], out.at[r, :], pair_send.at[u, j], pair_recv.at[u, j], sibling)

    def d2d_copy(s):
        return remote(theirs, d2d.at[s % 2], d2d_send.at[0], d2d_recv.at[s % 2], sibling)

    def first_copy(k):
        n = pl.ds(pl.multiple_of(k * (cols // PIECES), cols // PIECES), cols // PIECES)
        return remote(theirs.at[:, n], d2d.at[0, :, n], first_send.at[k], first_recv.at[k], sibling)

    n_steps = jnp.where(is_outer, max(STEPS[True]) + 1, max(STEPS[False]) + 1)
    most = max(max(STEPS[True]), max(STEPS[False])) + 1

    def step_units(s):
        picked = []
        for k in range(SLOT):
            q = {}
            for o in (True, False):
                table = []
                for i in range(most):
                    items = STEPS[o].get(i, [(0, 0 if o else 2)])
                    b, v = items[min(k, len(items) - 1)]
                    table.append(code(b, v))
                q[o] = select(s, table)
            picked.append(image(jnp.where(is_outer, q[True], q[False])))
        return picked

    def x_copy(start, n):
        return pltpu.make_async_copy(
            x.at[pl.ds(start, half), :], xb.at[pl.ds(n * half, half), :], x_sem.at[n])

    def x_copies(s):
        units = step_units(s)
        copies = []
        for n in range(2 * SLOT):
            c = core if n < SLOT else 1 - core
            copies.append(x_copy(pl.multiple_of(units[n % SLOT] * unit + c * half, half), n))
        return copies

    g_cols = wg.shape[1] // PIECES
    d_cols = cols // PIECES

    def w_copy(i, k):
        width = d_cols if i == 2 else g_cols
        n = pl.ds(pl.multiple_of(k * width, width), width)
        src, dst = ((wg, wg_v), (wu, wu_v), (wd, wd_v))[i]
        return pltpu.make_async_copy(src.at[:, n], dst.at[:, n], w_sem.at[i, k])

    def load(k):
        @pl.when(k < PIECES)
        def _():
            w_copy(0, k).start()
            w_copy(1, k).start()

        @pl.when((k >= PIECES) & (2 * (k - PIECES) < PIECES))
        def _():
            w_copy(2, 2 * (k - PIECES)).start()
            w_copy(2, 2 * (k - PIECES) + 1).start()

    load(jnp.int32(0))
    for copy in x_copies(jnp.int32(0)):
        copy.start()
    for k in range(1, AHEAD):
        load(jnp.int32(k))

    barrier = pltpu.get_barrier_semaphore()
    for o, here in ((True, is_outer), (False, is_inner)):
        @pl.when(here)
        def _(o=o):
            for to in (*ports[o], sibling):
                pl.semaphore_signal(barrier, inc=1, device_id={"tp": to}, device_id_type=MESH)
            pl.semaphore_wait(barrier, len(ports[o]) + 1)

    def send(o, e, r, j, src, dst, recv):
        remote(src, dst, send_sem.at[e, r % 2, j], recv, ports[o][e]).start()

    def free_slot(o, e, r, j):
        if any(k < r and (r - k) % 2 == 0 for k in SENDS[o, e]):
            slot = stage.at[e, r % 2, j]
            remote(slot, slot, send_sem.at[e, r % 2, j], ag_recv.at[0, 0], ports[o][e]).wait_send()

    def total(o, b, v, u, j, store):
        use = use_round(b, v)
        k = STEPS[o][use].index((b, v))
        r = pl.ds(pl.multiple_of(k * half + sub * j, sub), sub)
        places = []
        for c in children(b, v):
            ref, sem = landing(b, v, c, u, j)
            remote(ref, ref, send_sem.at[0, 0, 0], sem, sibling).wait_recv()
            places.append(ref)
        value = acc[r, :] + d2d[use % 2, r, :].astype(F32)
        for ref in places:
            value = value + ref[...].astype(F32)
        store[...] = value.astype(BF16)

    def comm(o, r, j):
        nodes = [(b, v) for b in range(len(TREES)) for v in NODES if outer(v) == o]
        for b, v in nodes:
            root, parent, up, down = TREES[b]
            if v != root and down[v] == r - 1:
                u = image(code(b, v))
                mine = out.at[piece(u, j), :]
                remote(mine, mine, send_sem.at[0, 0, 0], ag_recv.at[u, j], sibling).wait_recv()
                pair_copy(u, j).start()
        for b, v in nodes:
            if v == TREES[b][0] and use_round(b, v) == r:
                u = image(code(b, v))
                total(o, b, v, u, j, out.at[piece(u, j), :])
                pair_copy(u, j).start()
        for b, v in nodes:
            root, parent, up, down = TREES[b]
            for w in children(b, v):
                if down[w] == r:
                    u = image(code(b, v))
                    e = port_of(v, w)
                    free_slot(o, e, r, j)
                    r_out = out.at[piece(u, j), :]
                    send(o, e, r, j, r_out, r_out, ag_recv.at[u, j])
            if v != root and up[v] == r:
                u = image(code(b, v))
                e = port_of(v, parent[v])
                free_slot(o, e, r, j)
                slot = stage.at[e, r % 2, j]
                total(o, b, v, u, j, slot)
                send(o, e, r, j, slot, *landing(b, parent[v], v, u, j))

    def gate_up(s):
        for n in range(2 * SLOT):
            x_copy(0, n).wait()

        def hidden(n):
            gate = jnp.dot(xb[...], wg_v[:, n], preferred_element_type=F32)
            up = jnp.dot(xb[...], wu_v[:, n], preferred_element_type=F32)
            hid[:, n] = (jax.nn.silu(gate) * up).astype(BF16)

        @pl.when(s == 0)
        def _():
            def part(k, carry):
                w_copy(0, k).wait()
                w_copy(1, k).wait()
                load(k + AHEAD)
                hidden(pl.ds(pl.multiple_of(k * g_cols, g_cols), g_cols))
                return carry

            lax.fori_loop(0, PIECES, part, None)

        @pl.when(s > 0)
        def _():
            hidden(slice(None))

        @pl.when(s + 1 < n_steps)
        def _():
            for copy in x_copies(s + 1):
                copy.start()

    def down_proj(s):
        def term(n):
            value = jnp.dot(hid[...], wd_v[:, n], preferred_element_type=F32)
            acc[:, n] = value[:SLOT * half]
            theirs[:, n] = value[SLOT * half:].astype(BF16)

        @pl.when(s == 0)
        def _():
            def part(k, carry):
                w_copy(2, k).wait()
                term(pl.ds(pl.multiple_of(k * d_cols, d_cols), d_cols))
                first_copy(k).start()
                return carry

            lax.fori_loop(0, PIECES, part, None)

        @pl.when(s > 0)
        def _():
            @pl.when(s == 1)
            def _():
                for k in range(PIECES):
                    first_copy(k).wait_send()

            @pl.when(s > 1)
            def _():
                d2d_copy(s - 1).wait_send()

            n_cols = cols

            def part(k, carry):
                term(pl.ds(pl.multiple_of(k * n_cols, n_cols), n_cols))
                return carry

            lax.fori_loop(0, cols // n_cols, part, None)
            d2d_copy(s).start()

    def round_(i, carry):
        r = i - 1
        s = r + 1

        @pl.when(r == 0)
        def _():
            for k in range(PIECES):
                first_copy(k).wait_recv()

        @pl.when((r > 0) & (r < n_steps))
        def _():
            d2d_copy(r).wait_recv()

        def body(j, carry):
            for o, here in ((True, is_outer), (False, is_inner)):
                @pl.when(here)
                def _(o=o):
                    for first in range(0, ROUNDS + 1, GROUP):
                        @pl.when((r >= first) & (r < first + GROUP))
                        def _(first=first):
                            for k in range(first, min(first + GROUP, ROUNDS + 1)):
                                @pl.when(r == k)
                                def _(k=k):
                                    comm(o, k, j)

            @pl.when((s < n_steps) & (j == 0))
            def _():
                gate_up(s)

            @pl.when((s < n_steps) & (j == SUBS - 1))
            def _():
                down_proj(s)

            return carry

        return lax.fori_loop(0, SUBS, body, carry)

    lax.fori_loop(0, ROUNDS + 2, round_, None)

    for o, here in ((True, is_outer), (False, is_inner)):
        @pl.when(here)
        def _(o=o):
            for e in range(len(ports[o])):
                for parity in sorted({r % 2 for r in SENDS[o, e]}):
                    for j in range(SUBS):
                        slot = stage.at[e, parity, j]
                        remote(slot, slot, send_sem.at[e, parity, j], ag_recv.at[0, 0], ports[o][e]).wait_send()

    d2d_copy(n_steps - 1).wait_send()

    def drain(u, carry):
        for j in range(SUBS):
            pair_copy(u, j).wait_send()
            pair_copy(u, j, 1 - core).wait_recv()
        return carry

    lax.fori_loop(0, n_units, drain, None)


def copy_out_kernel(parts, src, dst, sem):
    n = src.shape[0] // parts
    copies = [
        pltpu.make_async_copy(src.at[pl.ds(k * n, n), :], dst.at[pl.ds(k * n, n), :], sem.at[k])
        for k in range(parts)
    ]
    for copy in copies:
        copy.start()
    for copy in copies:
        copy.wait()


def mlp(x, w_gate, w_up, w_down):
    rows, depth = x.shape
    ff = w_gate.shape[1]
    cols = w_down.shape[1]
    n_units = 4 * len(TREES)
    half = rows // n_units // 2
    sub = half // SUBS
    dma = pltpu.SemaphoreType.DMA
    any_spec = pl.BlockSpec(memory_space=pl.ANY)
    y = pl.pallas_call(
        block_kernel,
        out_shape=pltpu.VMEM((rows, cols), BF16),
        in_specs=[any_spec] * 4,
        out_specs=pl.BlockSpec(memory_space=pltpu.VMEM),
        scratch_shapes=[
            pltpu.VMEM((depth, ff), BF16),
            pltpu.VMEM((depth, ff), BF16),
            pltpu.VMEM((ff, cols), BF16),
            pltpu.VMEM((2 * SLOT * half, depth), BF16),
            pltpu.VMEM((SLOT * half, cols), F32),
            pltpu.VMEM((SLOT * half, cols), BF16),
            pltpu.VMEM((2, SLOT * half, cols), BF16),
            pltpu.VMEM((2 * SLOT * half, ff), BF16),
            pltpu.VMEM((3, 2, SUBS, sub, cols), BF16),
            pltpu.VMEM((N_EXTRA, half, cols), BF16),
            dma((3, PIECES)),
            dma((2 * SLOT,)),
            dma((PIECES,)),
            dma((PIECES,)),
            dma((1,)),
            dma((2,)),
            dma((3, 2, SUBS)),
            dma((n_units, SUBS)),
            dma((N_EXTRA, SUBS)),
            dma((n_units, SUBS)),
            dma((n_units, SUBS)),
            dma((n_units, SUBS)),
        ],
        compiler_params=pltpu.CompilerParams(
            collective_id=0, has_side_effects=True, vmem_limit_bytes=43 * 2**20),
        cost_estimate=pl.CostEstimate(
            flops=6 * rows * depth * ff, bytes_accessed=2 * (rows * depth + 3 * depth * ff),
            transcendentals=rows * ff),
        name="mlp_trees",
    )(x, w_gate, w_up, w_down)
    parts = 8
    return pl.pallas_call(
        functools.partial(copy_out_kernel, parts),
        out_shape=jax.ShapeDtypeStruct((rows, cols), BF16),
        in_specs=[pl.BlockSpec(memory_space=pltpu.VMEM)],
        out_specs=any_spec,
        scratch_shapes=[dma((parts,))],
        compiler_params=pltpu.CompilerParams(vmem_limit_bytes=2**20),
        name="copy_out",
    )(y)


def solution(mesh):
    return jax.shard_map(
        mlp,
        mesh=mesh,
        in_specs=(P("dp", None), P(None, "tp"), P(None, "tp"), P("tp", None)),
        out_specs=P("dp", None),
        check_vma=False,
    )
```
